256 devices in a mesh: seq: 32 (over x_lo, z, core), head: 8 (over y, x_hi).
Axes of the slice: x: 4 (x_hi: 2, x_lo: 2; x = x_hi * 2 + x_lo), y: 4, z: 8, core: 2. Of those that a mesh axis runs over, the one named last changes fastest.
Arguments:
- query_rows: bfloat16 [6144, 2048], P('seq', 'head'), may hold values from -6 to 6
- key_rows: bfloat16 [6144, 2048], P('seq', 'head'), may hold values from -6 to 6
- value_rows: bfloat16 [6144, 2048], P('seq', 'head'), may hold values from -6 to 6
- grad_output: bfloat16 [6144, 2048], P('seq', 'head'), may hold values from -6 to 6
- positions: int32 [6144], P('seq'), may hold values from 0 to 6143, each once
Outputs:
- grad_query: bfloat16 [6144, 2048], P(('seq', 'head'))
- grad_keys: bfloat16 [6144, 2048], P('seq', 'head')
- grad_values: bfloat16 [6144, 2048], P('seq', 'head')
The draws below stay inside these ranges and needn't reach their ends.
Inputs may be any that keep to these rules, and one draw needn't show every extreme that they name: `positions`: each number from 0 to 6143 appears once.
All inputs are finite; a program needn't handle non-finite values.
Results may differ from the reference program's by a relative error of at most 0.012.
Values may be sent and summed in bfloat16 or wider, within the bound.
No kernel may reach another device: no remote copies, remote signals or barrier semaphores. Data moves between devices by JAX's collectives and lax.ppermute only.
A program may use at most 128 MiB of HBM per device.

```python
import jax
import jax.numpy as jnp
from jax import lax

HEADS = 16
HEAD_DIM = 128
TOKENS = 6144


def base_rows(key, salt):
    noise_key = jax.random.fold_in(jax.random.fold_in(key, salt), 0)
    drawn = jax.random.normal(noise_key, (TOKENS, HEADS * HEAD_DIM), jnp.float32)
    return jnp.clip(drawn, -6.0, 6.0)


def draw_query_rows(key, part):
    drawn = base_rows(key, 1)
    return drawn.astype(jnp.bfloat16)


def draw_key_rows(key, part):
    drawn = base_rows(key, 2)
    return drawn.astype(jnp.bfloat16)


def block_levels(rng, shape, shards, smallest, high):
    def one(position, parts):
        heights = jax.random.uniform(jax.random.fold_in(jax.random.fold_in(rng, 6), position), (parts,), jnp.float32, smallest / len(shards), high / len(shards))
        return jnp.repeat(jnp.exp(heights), shape[position] // parts).reshape((-1,) + (1,) * (len(shape) - position - 1))

    factor_of = one(*shards[0])
    for cut in shards[1:]:
        factor_of = factor_of * one(*cut)
    return factor_of


def scatter_about(rng, extent, spread, most, cuts=(), held_as=jnp.bfloat16):
    entries = jax.random.normal(rng, extent, jnp.float32) * spread
    if len(cuts) > 0:
        entries = block_levels(rng, extent, cuts, -0.22, 0.18) * entries
    return jnp.clip(entries, min=-most, max=most).astype(held_as)


def setup_inputs(seed: int = 0) -> dict:
    streams_of = jax.random.split(jax.random.key(seed), 6)
    return {
        "query_rows": draw_query_rows(jax.random.fold_in(streams_of[5], 71), 0),
        "key_rows": draw_key_rows(jax.random.fold_in(streams_of[5], 71), 0),
        "value_rows": scatter_about(streams_of[2], (TOKENS, HEADS * HEAD_DIM), 1.0, 6.0, ((0, 32), (1, 8))),
        "grad_output": scatter_about(streams_of[3], (TOKENS, HEADS * HEAD_DIM), 1.0, 6.0, ((0, 32), (1, 8))),
        "positions": jax.random.permutation(streams_of[4], TOKENS).astype(jnp.int32),
    }


def reference(query_rows, key_rows, value_rows, grad_output, positions):
    tokens = query_rows.shape[0]
    scaling = HEAD_DIM ** -0.5
    allowed = positions[None, :] <= positions[:, None]

    def per_head(matrix):
        return jnp.swapaxes(matrix.reshape(tokens, HEADS, HEAD_DIM), 0, 1)

    def back_rows(matrix):
        return jnp.swapaxes(matrix, 0, 1).reshape(tokens, HEADS * HEAD_DIM)

    def one_head(head_items):
        query_full = head_items[0].astype(jnp.float32)
        key_full = head_items[1].astype(jnp.float32)
        value_full = head_items[2].astype(jnp.float32)
        grad_full = head_items[3].astype(jnp.float32)
        highest = lax.Precision.HIGHEST
        scores = jnp.dot(query_full, key_full.T, precision=highest) * scaling
        masked = jnp.where(allowed, scores, -1.0e30)
        top_score = jnp.max(masked, axis=1)
        denominator = jnp.sum(jnp.where(allowed, jnp.exp(masked - top_score[:, None]), 0.0), axis=1)
        log_total = top_score + jnp.log(denominator)
        probabilities = jnp.where(allowed, jnp.exp(masked - log_total[:, None]), 0.0)
        weights = probabilities.astype(jnp.bfloat16).astype(jnp.float32)
        grad_probs = jnp.dot(grad_full, value_full.T, precision=highest)
        row_delta = jnp.sum(probabilities * grad_probs, axis=1)
        grad_value = jnp.dot(weights.T, grad_full, precision=highest)
        grad_scores = (probabilities * (grad_probs - row_delta[:, None]) * scaling).astype(jnp.bfloat16).astype(jnp.float32)
        grad_query = jnp.dot(grad_scores, key_full, precision=highest)
        grad_key = jnp.dot(grad_scores.T, query_full, precision=highest)
        return grad_query.astype(jnp.bfloat16), grad_key.astype(jnp.bfloat16), grad_value.astype(jnp.bfloat16)

    grad_query, grad_keys, grad_values = lax.map(one_head, (per_head(query_rows), per_head(key_rows), per_head(value_rows), per_head(grad_output)))
    return back_rows(grad_query), back_rows(grad_keys), back_rows(grad_values)
```

```python
import functools

import jax
import jax.numpy as jnp
from jax import lax
from jax.experimental import pallas as pl
from jax.experimental.pallas import tpu as pltpu
from jax.sharding import PartitionSpec as P

HEAD_DIM = 128
ROWS = 192
QUAD = 4
LOG2E = 1.4426950408889634
SCALE = HEAD_DIM**-0.5
LOW = -1e30
F32 = jnp.float32
BF16 = jnp.bfloat16


def z_of(j, half):
    return 2 * j + half


def perm(xor_x=0, xor_j=0, xor_half=0, xor_core=0):
    pairs = []
    for x in range(2):
        for j in range(4):
            for h in range(2):
                for c in range(2):
                    src = x * 16 + z_of(j, h) * 2 + c
                    dst = (x ^ xor_x) * 16 + z_of(j ^ xor_j, h ^ xor_half) * 2 + (c ^ xor_core)
                    pairs.append((src, dst))
    return pairs


def move(value, **how):
    return lax.ppermute(value, "seq", perm(**how))


def pack(first, second, positions):
    high = (positions // 128).astype(BF16)
    low = (positions % 128).astype(BF16)
    tags = jnp.stack([high, low])
    tags = jnp.pad(tags, ((0, 0), (0, 2 * HEAD_DIM - ROWS)))
    tags = jnp.broadcast_to(tags[:, None, :], (2, 8, 2 * HEAD_DIM)).reshape(16, 2 * HEAD_DIM)
    return jnp.concatenate([first, second, tags], axis=0)


def places(packed_ref):
    tags = packed_ref[2 * ROWS : 2 * ROWS + 16, :].astype(F32)
    return tags[0:8] * 128.0 + tags[8:16]


def assemble(slot_ref, query_refs, key_refs, queries, grads, keys, values, query_pos, key_pos):
    mine = slot_ref[0]
    pos = []
    for t in range(QUAD):
        start = pl.multiple_of((mine ^ t) * ROWS, 64)
        queries[pl.ds(start, ROWS), :] = query_refs[t][0:ROWS, :]
        grads[pl.ds(start, ROWS), :] = query_refs[t][ROWS : 2 * ROWS, :]
        pos.append(places(query_refs[t]))
    ordered = []
    for a in range(QUAD):
        row = pos[0]
        for t in range(1, QUAD):
            row = jnp.where((mine ^ t) == a, pos[t], row)
        ordered.append(row)
    lane = lax.broadcasted_iota(jnp.int32, (8, 128), 1)
    for pair in range(2):
        left, right = ordered[2 * pair], ordered[2 * pair + 1]
        turned_a = pltpu.roll(right[:, 0:128], 64, 1)
        turned_b = pltpu.roll(right[:, 128:256], 64, 1)
        base = pair * 384
        query_pos[:, base : base + 128] = left[:, 0:128]
        query_pos[:, base + 128 : base + 256] = jnp.where(lane < 64, left[:, 128:256], turned_a)
        query_pos[:, base + 256 : base + 384] = jnp.where(lane < 64, turned_a, turned_b)
    for n in range(8):
        keys[n * ROWS : (n + 1) * ROWS, :] = key_refs[n][0:ROWS, :]
        values[n * ROWS : (n + 1) * ROWS, :] = key_refs[n][ROWS : 2 * ROWS, :]
        row = places(key_refs[n])
        tall = jnp.concatenate([row] * 16, axis=0)
        key_pos[n * ROWS : n * ROWS + 128, :] = jnp.transpose(tall[:, 0:128])
        key_pos[n * ROWS + 128 : (n + 1) * ROWS, :] = jnp.transpose(tall[:, 128:256])[0:64]


TILE = 256
QUERIES = QUAD * ROWS
KEYS = 8 * ROWS


def dot_t(a, b):
    return lax.dot_general(a, b, (((1,), (1,)), ((), ())), preferred_element_type=F32)


def masked_scores(queries, keys, query_pos, key_pos, head, start, wide):
    cols = slice(head * 128, (head + 1) * 128)
    s = dot_t(keys[pl.ds(start, TILE), cols], queries[:, cols])
    s = s.reshape(TILE // 8, 8, QUERIES) * (SCALE * LOG2E)
    place = key_pos[pl.ds(start, TILE), :].reshape(TILE // 8, 8, 128)
    place = jnp.concatenate([place] * (QUERIES // 128), axis=2)
    return jnp.where(place <= query_pos[...][None], s, LOW)


def stats_kernel(slot_ref, *refs):
    query_refs, key_refs, out_ref = refs[0:4], refs[4:12], refs[12]
    queries, grads, keys, values, query_pos, key_pos = refs[13:]
    assemble(slot_ref, query_refs, key_refs, queries, grads, keys, values, query_pos, key_pos)
    for head in range(2):
        cols = slice(head * 128, (head + 1) * 128)

        def turn(i, running):
            top, total, delta = running
            start = pl.multiple_of(i * TILE, TILE)
            s = masked_scores(queries, keys, query_pos, key_pos, head, start, None)
            g = dot_t(values[pl.ds(start, TILE), cols], grads[:, cols])
            g = g.reshape(TILE // 8, 8, QUERIES)
            new = jnp.maximum(top, jnp.max(s, axis=0))
            shrink = jnp.exp2(top - new)
            p = jnp.exp2(s - new[None])
            total = total * shrink + jnp.sum(p, axis=0)
            delta = delta * shrink + jnp.sum(p * g, axis=0)
            return new, total, delta

        start = (
            jnp.full((8, QUERIES), LOW, F32),
            jnp.zeros((8, QUERIES), F32),
            jnp.zeros((8, QUERIES), F32),
        )
        top, total, delta = lax.fori_loop(0, KEYS // TILE, turn, start)
        best = jnp.max(top, axis=0, keepdims=True)
        shrink = jnp.exp2(top - best)
        out_ref[3 * head : 3 * head + 1, :] = best
        out_ref[3 * head + 1 : 3 * head + 2, :] = jnp.sum(total * shrink, axis=0, keepdims=True)
        out_ref[3 * head + 2 : 3 * head + 3, :] = jnp.sum(delta * shrink, axis=0, keepdims=True)
    out_ref[6:8, :] = jnp.zeros((2, QUERIES), F32)


def grads_kernel(slot_ref, *refs):
    query_refs, key_refs, stat_refs = refs[0:4], refs[4:12], refs[12:16]
    own_query, query_outs = refs[16], refs[17:20]
    own_keys, far_keys = refs[20], refs[21]
    queries, grads, keys, values, query_pos, key_pos, keys_t, query_sum = refs[22:]
    assemble(slot_ref, query_refs, key_refs, queries, grads, keys, values, query_pos, key_pos)
    mine = slot_ref[0]
    stats = [r[...] for r in stat_refs]
    for head in range(2):
        cols = slice(head * 128, (head + 1) * 128)
        keys_t[...] = jnp.transpose(keys[:, cols])
        tops = [s[3 * head : 3 * head + 1] for s in stats]
        best = functools.reduce(jnp.maximum, tops)
        shrinks = [jnp.exp2(t - best) for t in tops]
        total = sum(s[3 * head + 1 : 3 * head + 2] * w for s, w in zip(stats, shrinks))
        delta = sum(s[3 * head + 2 : 3 * head + 3] * w for s, w in zip(stats, shrinks)) / total
        log_total = jnp.broadcast_to(best + jnp.log2(total), (8, QUERIES))
        delta = jnp.broadcast_to(delta, (8, QUERIES))
        query_sum[...] = jnp.zeros_like(query_sum)
        for n in range(KEYS // TILE):
            start = n * TILE
            s = masked_scores(queries, keys, query_pos, key_pos, head, start, None)
            g = dot_t(values[pl.ds(start, TILE), cols], grads[:, cols])
            g = g.reshape(TILE // 8, 8, QUERIES)
            p = jnp.exp2(s - log_total[None])
            d = (p * (g - delta[None])).reshape(TILE, QUERIES).astype(BF16)
            p = p.reshape(TILE, QUERIES).astype(BF16)
            grad_value = jnp.dot(p, grads[:, cols], preferred_element_type=F32)
            grad_key = jnp.dot(d, queries[:, cols], preferred_element_type=F32) * SCALE
            query_sum[...] += jnp.dot(keys_t[:, start : start + TILE], d, preferred_element_type=F32)
            at = 0
            while at < TILE:
                row = start + at
                chunk, inside = row // ROWS, row % ROWS
                size = min(TILE - at, ROWS - inside)
                target = own_keys if chunk < 4 else far_keys
                where = chunk % 4
                target[where, inside : inside + size, cols] = grad_key[at : at + size].astype(target.dtype)
                target[where, ROWS + inside : ROWS + inside + size, cols] = grad_value[
                    at : at + size
                ].astype(target.dtype)
                at += size
        turned = jnp.transpose(query_sum[...]) * SCALE
        query_rows = refs[-2] if False else turned
        for a in range(QUAD):
            part = query_rows[a * ROWS : (a + 1) * ROWS]

            @pl.when(mine == a)
            def _():
                own_query[:, cols] = part

            for t in range(1, QUAD):

                @pl.when((mine ^ t) == a)
                def _():
                    query_outs[t - 1][:, cols] = part.astype(BF16)


def in_vmem(n):
    return [pl.BlockSpec(memory_space=pltpu.VMEM)] * n


def scratch():
    return [
        pltpu.VMEM((QUERIES, 256), BF16),
        pltpu.VMEM((QUERIES, 256), BF16),
        pltpu.VMEM((KEYS, 256), BF16),
        pltpu.VMEM((KEYS, 256), BF16),
        pltpu.VMEM((8, QUERIES), F32),
        pltpu.VMEM((KEYS, 128), F32),
    ]


def local(query_rows, key_rows, value_rows, grad_output, positions):
    place = lax.axis_index("seq")
    slot = ((place // 4) % 4).astype(jnp.int32).reshape(1)
    query_pack = pack(query_rows, grad_output, positions)
    key_pack = pack(key_rows, value_rows, positions)
    key_x = move(key_pack, xor_x=1)
    key_z = move(key_pack, xor_half=1)
    query_packs = [query_pack] + [move(query_pack, xor_j=t) for t in (2, 1, 3)]
    query_packs = [query_packs[0], query_packs[2], query_packs[1], query_packs[3]]
    key_xz = move(key_z, xor_x=1)
    key_packs = [key_pack, key_x, key_z, key_xz]
    key_packs = key_packs + [move(k, xor_core=1) for k in key_packs]

    params = pltpu.CompilerParams(vmem_limit_bytes=48 * 1024 * 1024)
    smem = [pl.BlockSpec(memory_space=pltpu.SMEM)]
    stats = pl.pallas_call(
        stats_kernel,
        out_shape=jax.ShapeDtypeStruct((8, QUERIES), F32),
        in_specs=smem + in_vmem(12),
        out_specs=pl.BlockSpec(memory_space=pltpu.VMEM),
        scratch_shapes=scratch(),
        compiler_params=params,
        cost_estimate=pl.CostEstimate(flops=3 * 10**9, bytes_accessed=3 * 10**6, transcendentals=0),
        name="stats",
    )(slot, *query_packs, *key_packs)
    all_stats = [stats] + [move(stats, xor_j=t) for t in range(1, QUAD)]
    outs = pl.pallas_call(
        grads_kernel,
        out_shape=(
            jax.ShapeDtypeStruct((ROWS, 256), F32),
            *[jax.ShapeDtypeStruct((ROWS, 256), BF16)] * 3,
            jax.ShapeDtypeStruct((4, 2 * ROWS, 256), F32),
            jax.ShapeDtypeStruct((4, 2 * ROWS, 256), BF16),
        ),
        in_specs=smem + in_vmem(16),
        out_specs=tuple(in_vmem(6)),
        scratch_shapes=scratch() + [pltpu.VMEM((128, KEYS), BF16), pltpu.VMEM((128, QUERIES), F32)],
        compiler_params=params,
        cost_estimate=pl.CostEstimate(flops=6 * 10**9, bytes_accessed=6 * 10**6, transcendentals=0),
        name="grads",
    )(slot, *query_packs, *key_packs, *all_stats)
    own_query, query_outs, own_keys, far_keys = outs[0], outs[1:4], outs[4], outs[5]
    query_terms = [move(query_outs[t - 1], xor_j=t) for t in range(1, QUAD)]
    near = own_keys + move(far_keys, xor_core=1).astype(F32)
    back_x = move(near[1].astype(BF16), xor_x=1)
    back_z = move(near[2].astype(BF16), xor_half=1)
    back_xz = move(near[3].astype(BF16), xor_x=1, xor_half=1)
    grad_query = own_query + sum(t.astype(F32) for t in query_terms)
    regrouped = lax.all_to_all(grad_query.astype(BF16), "head", split_axis=0, concat_axis=1, tiled=True)
    both = near[0] + back_x.astype(F32) + back_z.astype(F32) + back_xz.astype(F32)
    both = both.astype(BF16)
    return regrouped, both[:ROWS], both[ROWS:]


def solution(mesh):
    placed = (P("seq", "head"), P("seq", "head"), P("seq", "head"), P("seq", "head"), P("seq"))
    return jax.shard_map(
        local,
        mesh=mesh,
        in_specs=placed,
        out_specs=(P(("seq", "head"), None), P("seq", "head"), P("seq", "head")),
        check_vma=False,
    )
```

```python
import functools

import jax
import jax.numpy as jnp
from jax import lax
from jax.experimental import pallas as pl
from jax.experimental.pallas import tpu as pltpu
from jax.sharding import PartitionSpec as P

HEAD_DIM = 128
ROWS = 192
BOTH = 2 * ROWS
QUAD = 4
QUERIES = QUAD * BOTH
HALF_KEYS = 2 * BOTH
TILE = 256
FIRST_MIB = 16
GRADS_MIB = 16
LOG2E = 1.4426950408889634
SCALE = HEAD_DIM**-0.5
LOW = -1e30
F32 = jnp.float32
BF16 = jnp.bfloat16


def z_of(j, half):
    return 2 * j + half


def perm(xor_x=0, xor_j=0, xor_half=0, xor_core=0):
    pairs = []
    for x in range(2):
        for j in range(4):
            for h in range(2):
                for c in range(2):
                    src = x * 16 + z_of(j, h) * 2 + c
                    dst = (x ^ xor_x) * 16 + z_of(j ^ xor_j, h ^ xor_half) * 2 + (c ^ xor_core)
                    pairs.append((src, dst))
    return pairs


def move(value, **how):
    return lax.ppermute(value, "seq", perm(**how))


def near_move(value, t):
    return move(value, xor_x=t // 2, xor_half=t % 2)


def pack(first, second, positions):
    high = (positions // 128).astype(BF16)
    low = (positions % 128).astype(BF16)
    tags = jnp.stack([high, low])
    tags = jnp.pad(tags, ((0, 0), (0, 2 * HEAD_DIM - ROWS)))
    tags = jnp.broadcast_to(tags[:, None, :], (2, 8, 2 * HEAD_DIM)).reshape(16, 2 * HEAD_DIM)
    return jnp.concatenate([first, second, tags], axis=0)


def places(packed_ref):
    tags = packed_ref[BOTH : BOTH + 16, :].astype(F32)
    return tags[0:8] * 128.0 + tags[8:16]


def split(packed_ref, cols, first, second, start):
    first[pl.ds(start, ROWS), :] = packed_ref[0:ROWS, cols]
    second[pl.ds(start, ROWS), :] = packed_ref[ROWS:BOTH, cols]


def head_cols(core):
    return pl.ds(pl.multiple_of(core * HEAD_DIM, HEAD_DIM), HEAD_DIM)


def take_queries(where_ref, refs, queries, grads, query_pos):
    mine, core = where_ref[0], where_ref[1]
    lane = lax.broadcasted_iota(jnp.int32, (8, 128), 1)
    for t in range(QUAD):
        chip = (mine ^ t) * BOTH
        for far in range(2):
            start = pl.multiple_of(chip + (core ^ far) * ROWS, 64)
            split(refs[2 * t + far], head_cols(core), queries, grads, start)
        own, other = places(refs[2 * t]), places(refs[2 * t + 1])
        left = jnp.where(core == 0, own, other)
        right = jnp.where(core == 0, other, own)
        turned_a = pltpu.roll(right[:, 0:128], 64, 1)
        turned_b = pltpu.roll(right[:, 128:256], 64, 1)
        row = jnp.concatenate(
            [left[:, 0:128], jnp.where(lane < 64, left[:, 128:256], turned_a), jnp.where(lane < 64, turned_a, turned_b)],
            axis=1,
        )
        query_pos[:, pl.ds(pl.multiple_of(chip, 128), BOTH)] = row


def take_keys(where_ref, refs, keys, values, key_pos):
    core = where_ref[1]
    for n in range(4):
        start = pl.multiple_of((n // 2) * BOTH + (core ^ (n % 2)) * ROWS, 64)
        split(refs[n], head_cols(core), keys, values, start)
        tall = jnp.concatenate([places(refs[n])] * 16, axis=0)
        key_pos[pl.ds(start, 128), :] = jnp.transpose(tall[:, 0:128])
        key_pos[pl.ds(start + 128, 64), :] = jnp.transpose(tall[:, 128:256])[0:64]


def dot_t(a, b):
    return lax.dot_general(a, b, (((1,), (1,)), ((), ())), preferred_element_type=F32)


def masked_scores(queries, keys, query_pos, key_pos, start):
    s = dot_t(keys[pl.ds(start, TILE), :], queries[...])
    s = s.reshape(TILE // 8, 8, QUERIES) * (SCALE * LOG2E)
    place = key_pos[pl.ds(start, TILE), :].reshape(TILE // 8, 8, 128)
    place = jnp.concatenate([place] * (QUERIES // 128), axis=2)
    return jnp.where(place <= query_pos[...][None], s, LOW)


def sweep(queries, grads, query_pos, keys, values, key_pos, scores, products, running):
    def turn(i, running):
        top, total, delta = running
        start = pl.multiple_of(i * TILE, TILE)
        s = masked_scores(queries, keys, query_pos, key_pos, start)
        g = dot_t(values[pl.ds(start, TILE), :], grads[...])
        scores[pl.ds(start, TILE), :] = s.reshape(TILE, QUERIES)
        products[pl.ds(start, TILE), :] = g
        g = g.reshape(TILE // 8, 8, QUERIES)
        new = jnp.maximum(top, jnp.max(s, axis=0))
        shrink = jnp.exp2(top - new)
        p = jnp.exp2(s - new[None])
        total = total * shrink + jnp.sum(p, axis=0)
        delta = delta * shrink + jnp.sum(p * g, axis=0)
        return new, total, delta

    return lax.fori_loop(0, HALF_KEYS // TILE, turn, running)


def first_kernel(where_ref, *refs):
    query_refs, key_refs = refs[0:8], refs[8:12]
    queries, grads, query_pos, keys, scores, products, out, values, key_pos = refs[12:]
    take_queries(where_ref, query_refs, queries, grads, query_pos)
    take_keys(where_ref, key_refs, keys, values, key_pos)
    start = (
        jnp.full((8, QUERIES), LOW, F32),
        jnp.zeros((8, QUERIES), F32),
        jnp.zeros((8, QUERIES), F32),
    )
    found = sweep(queries, grads, query_pos, keys, values, key_pos, scores, products, start)
    for n in range(3):
        out[n] = found[n]


def second_kernel(where_ref, *refs):
    queries, grads, query_pos, before = refs[0:4]
    key_refs = refs[4:8]
    keys, scores, products, out, values, key_pos = refs[8:]
    take_keys(where_ref, key_refs, keys, values, key_pos)
    running = (before[0], before[1], before[2])
    top, total, delta = sweep(queries, grads, query_pos, keys, values, key_pos, scores, products, running)
    best = jnp.max(top, axis=0, keepdims=True)
    shrink = jnp.exp2(top - best)
    out[0:1, :] = best
    out[1:2, :] = jnp.sum(total * shrink, axis=0, keepdims=True)
    out[2:3, :] = jnp.sum(delta * shrink, axis=0, keepdims=True)
    out[3:8, :] = jnp.zeros((5, QUERIES), F32)


def grads_kernel(where_ref, *refs):
    queries, grads = refs[0:2]
    key_refs = refs[2:8]
    stat_refs = refs[8:12]
    own_query, query_outs = refs[12], refs[13:16]
    own_keys, key_outs = refs[16], refs[17:20]
    query_sum, query_rows = refs[20:]
    mine = where_ref[0]
    stats = [r[...] for r in stat_refs]
    tops = [s[0:1] for s in stats]
    best = functools.reduce(jnp.maximum, tops)
    shrinks = [jnp.exp2(t - best) for t in tops]
    total = sum(s[1:2] * w for s, w in zip(stats, shrinks))
    delta = sum(s[2:3] * w for s, w in zip(stats, shrinks)) / total
    log_total = jnp.broadcast_to(best + jnp.log2(total), (8, QUERIES))
    delta = jnp.broadcast_to(delta, (8, QUERIES))
    query_sum[...] = jnp.zeros_like(query_sum)
    for part in range(2):
        keys, scores, products = key_refs[3 * part : 3 * part + 3]
        for n in range(HALF_KEYS // TILE):
            start = n * TILE
            s = scores[start : start + TILE, :].reshape(TILE // 8, 8, QUERIES)
            g = products[start : start + TILE, :].reshape(TILE // 8, 8, QUERIES)
            p = jnp.exp2(s - log_total[None])
            d = (p * (g - delta[None])).reshape(TILE, QUERIES).astype(BF16)
            p = p.reshape(TILE, QUERIES).astype(BF16)
            grad_value = jnp.dot(p, grads[...], preferred_element_type=F32)
            grad_key = jnp.dot(d, queries[...], preferred_element_type=F32) * SCALE
            keys_t = jnp.transpose(keys[start : start + TILE, :])
            query_sum[...] += jnp.dot(keys_t, d, preferred_element_type=F32)
            at = 0
            while at < TILE:
                row = start + at
                chunk, inside = 2 * part + row // BOTH, row % BOTH
                size = min(TILE - at, BOTH - inside)
                target = own_keys if chunk == 0 else key_outs[chunk - 1]
                target[inside : inside + size, :] = grad_key[at : at + size].astype(target.dtype)
                target[BOTH + inside : BOTH + inside + size, :] = grad_value[at : at + size].astype(target.dtype)
                at += size
    query_rows[...] = jnp.transpose(query_sum[...]) * SCALE
    for t in range(QUAD):
        rows = query_rows[pl.ds(pl.multiple_of((mine ^ t) * BOTH, BOTH), BOTH), :]
        if t == 0:
            own_query[...] = rows
        else:
            query_outs[t - 1][...] = rows.astype(BF16)


def in_vmem(n):
    return [pl.BlockSpec(memory_space=pltpu.VMEM)] * n


def shaped(*shape, dtype=BF16):
    return jax.ShapeDtypeStruct(shape, dtype)


def call(kernel, outs, scratch, flops, mib, where, *args):
    return pl.pallas_call(
        kernel,
        out_shape=tuple(outs),
        in_specs=[pl.BlockSpec(memory_space=pltpu.SMEM)] + in_vmem(len(args)),
        out_specs=tuple(in_vmem(len(outs))),
        scratch_shapes=scratch,
        compiler_params=pltpu.CompilerParams(vmem_limit_bytes=mib * 1024 * 1024),
        cost_estimate=pl.CostEstimate(flops=flops, bytes_accessed=4 * 10**6, transcendentals=0),
    )(where, *args)


def heads_of_own_rows(value, core):
    kept = lax.dynamic_index_in_dim(value, core, 0, False)
    sent = lax.dynamic_index_in_dim(value, 1 - core, 0, False)
    came = move(sent, xor_core=1)
    first = jnp.where(core == 0, kept, came)
    last = jnp.where(core == 0, came, kept)
    return jnp.concatenate([first, last], axis=-1)


def body(query_rows, key_rows, value_rows, grad_output, positions):
    place = lax.axis_index("seq")
    core = place % 2
    where = jnp.stack([(place // 16) * 2 + (place // 2) % 2, core]).astype(jnp.int32)
    key_pack = pack(key_rows, value_rows, positions)
    query_pack = pack(query_rows, grad_output, positions)
    key_packs = [key_pack] + [move(key_pack, xor_j=t) for t in range(1, 4)]
    query_z = move(query_pack, xor_half=1)
    query_x = move(query_pack, xor_x=1)
    query_packs = [query_pack, query_z, query_x, move(query_z, xor_x=1)]
    all_keys = [v for k in key_packs for v in (k, move(k, xor_core=1))]
    all_queries = [v for q in query_packs for v in (q, move(q, xor_core=1))]

    rows = [shaped(QUERIES, 128), shaped(QUERIES, 128), shaped(8, QUERIES, dtype=F32)]
    tall = shaped(HALF_KEYS, QUERIES, dtype=F32)
    half = [shaped(HALF_KEYS, 128), tall, tall]
    spare = [pltpu.VMEM((HALF_KEYS, 128), BF16), pltpu.VMEM((HALF_KEYS, 128), F32)]
    *taken, keys_a, scores_a, products_a, running = call(
        first_kernel, rows + half + [shaped(3, 8, QUERIES, dtype=F32)], spare, 2 * 10**9, FIRST_MIB, where,
        *all_queries, *all_keys[:4],
    )
    keys_b, scores_b, products_b, stats = call(
        second_kernel, half + [shaped(8, QUERIES, dtype=F32)], spare, 2 * 10**9, FIRST_MIB, where,
        *taken, running, *all_keys[4:],
    )
    all_stats = [stats] + [near_move(stats, t) for t in range(1, QUAD)]
    outs = call(
        grads_kernel,
        [shaped(BOTH, 128, dtype=F32)] + [shaped(BOTH, 128)] * 3
        + [shaped(2 * BOTH, 128, dtype=F32)] + [shaped(2 * BOTH, 128)] * 3,
        [pltpu.VMEM((128, QUERIES), F32), pltpu.VMEM((QUERIES, 128), F32)], 6 * 10**9, GRADS_MIB, where,
        *taken[:2], keys_a, scores_a, products_a, keys_b, scores_b, products_b, *all_stats,
    )
    own_query, query_outs, own_keys, key_outs = outs[0], outs[1:4], outs[4], outs[5:8]
    query_terms = [near_move(query_outs[t - 1], t) for t in range(1, QUAD)]
    key_terms = [move(key_outs[t - 1], xor_j=t) for t in range(1, QUAD)]
    grad_query = (own_query + sum(t.astype(F32) for t in query_terms)).astype(BF16)
    grad_query = heads_of_own_rows(grad_query.reshape(2, ROWS, 128), core)
    regrouped = lax.all_to_all(grad_query.reshape(8, 24, 256), "head", 0, 0)
    regrouped = jnp.swapaxes(regrouped, 0, 1).reshape(24, 2048)
    both = (own_keys + sum(t.astype(F32) for t in key_terms)).astype(BF16)
    both = both.reshape(2, 2, ROWS, 128)
    grad_keys, grad_values = heads_of_own_rows(jnp.swapaxes(both, 0, 1), core)
    return regrouped, grad_keys, grad_values


def solution(mesh):
    placed = (P("seq", "head"), P("seq", "head"), P("seq", "head"), P("seq", "head"), P("seq"))
    return jax.shard_map(
        body,
        mesh=mesh,
        in_specs=placed,
        out_specs=(P(("seq", "head"), None), P("seq", "head"), P("seq", "head")),
        check_vma=False,
    )
```

```python
import functools

import jax
import jax.numpy as jnp
from jax import lax
from jax.experimental import pallas as pl
from jax.experimental.pallas import tpu as pltpu
from jax.sharding import PartitionSpec as P

HEAD_DIM = 128
ROWS = 192
TAGS = 16
BOTH = 2 * ROWS
QUAD = 4
QUERIES = QUAD * BOTH
MID, LAST = 3, 2
FIRST_MIB = 16
GRADS_MIB = 16
LOG2E = 1.4426950408889634
SCALE = HEAD_DIM**-0.5
LOW = -1e30
F32 = jnp.float32
BF16 = jnp.bfloat16


def z_of(j, half):
    return 2 * j + half


def perm(xor_x=0, xor_j=0, xor_half=0, xor_core=0):
    pairs = []
    for x in range(2):
        for j in range(4):
            for h in range(2):
                for c in range(2):
                    src = x * 16 + z_of(j, h) * 2 + c
                    dst = (x ^ xor_x) * 16 + z_of(j ^ xor_j, h ^ xor_half) * 2 + (c ^ xor_core)
                    pairs.append((src, dst))
    return pairs


def move(value, **how):
    return lax.ppermute(value, "seq", perm(**how))


def near_move(value, t):
    return move(value, xor_x=t // 2, xor_half=t % 2)


def pack(first, second, positions):
    high = (positions // 128).astype(BF16)
    low = (positions % 128).astype(BF16)
    tags = jnp.stack([high, low])
    tags = jnp.pad(tags, ((0, 0), (0, 2 * HEAD_DIM - ROWS)))
    tags = jnp.broadcast_to(tags[:, None, :], (2, 8, 2 * HEAD_DIM)).reshape(16, 2 * HEAD_DIM)
    return jnp.concatenate([tags, first, second], axis=0)


def places(packed_ref):
    tags = packed_ref[0:TAGS, :].astype(F32)
    return tags[0:8] * 128.0 + tags[8:16]


def split(packed_ref, cols, first, second, start):
    if isinstance(packed_ref, tuple):
        head, tail, base = *packed_ref, 0
    else:
        head, tail, base = packed_ref, packed_ref, TAGS + ROWS
    first[pl.ds(start, ROWS), :] = head[TAGS : TAGS + ROWS, cols]
    second[pl.ds(start, ROWS), :] = tail[base : base + ROWS, cols]


def head_cols(core):
    return pl.ds(pl.multiple_of(core * HEAD_DIM, HEAD_DIM), HEAD_DIM)


def take_queries(where_ref, refs, queries, grads, query_pos):
    mine, core = where_ref[0], where_ref[1]
    lane = lax.broadcasted_iota(jnp.int32, (8, 128), 1)
    for t in range(QUAD):
        chip = (mine ^ t) * BOTH
        for far in range(2):
            start = pl.multiple_of(chip + (core ^ far) * ROWS, 64)
            split(refs[2 * t + far], head_cols(core), queries, grads, start)
        own, other = places(refs[2 * t]), places(refs[2 * t + 1])
        left = jnp.where(core == 0, own, other)
        right = jnp.where(core == 0, other, own)
        turned_a = pltpu.roll(right[:, 0:128], 64, 1)
        turned_b = pltpu.roll(right[:, 128:256], 64, 1)
        row = jnp.concatenate(
            [left[:, 0:128], jnp.where(lane < 64, left[:, 128:256], turned_a), jnp.where(lane < 64, turned_a, turned_b)],
            axis=1,
        )
        query_pos[:, pl.ds(pl.multiple_of(chip, 128), BOTH)] = row


def take_keys(where_ref, refs, keys, values, key_pos):
    core = where_ref[1]
    for n in range(len(refs)):
        start = pl.multiple_of((n // 2) * BOTH + (core ^ (n % 2)) * ROWS, 64)
        split(refs[n], head_cols(core), keys, values, start)
        tagged = refs[n][0] if isinstance(refs[n], tuple) else refs[n]
        tall = jnp.concatenate([places(tagged)] * 16, axis=0)
        key_pos[pl.ds(start, 128), :] = jnp.transpose(tall[:, 0:128])
        key_pos[pl.ds(start + 128, 64), :] = jnp.transpose(tall[:, 128:256])[0:64]


def tile_of(keys):
    return 256 if keys.shape[0] % 256 == 0 else 192


def dot_t(a, b):
    return lax.dot_general(a, b, (((1,), (1,)), ((), ())), preferred_element_type=F32)


def masked_scores(queries, keys, query_pos, key_pos, start, tile):
    s = dot_t(keys[pl.ds(start, tile), :], queries[...])
    s = s.reshape(tile // 8, 8, QUERIES) * (SCALE * LOG2E)
    place = key_pos[pl.ds(start, tile), :].reshape(tile // 8, 8, 128)
    place = jnp.concatenate([place] * (QUERIES // 128), axis=2)
    return jnp.where(place <= query_pos[...][None], s, LOW)


def sweep(queries, grads, query_pos, keys, values, key_pos, scores, products, running):
    tile = tile_of(keys)

    def turn(i, running):
        top, total, delta = running
        start = pl.multiple_of(i * tile, tile)
        s = masked_scores(queries, keys, query_pos, key_pos, start, tile)
        g = dot_t(values[pl.ds(start, tile), :], grads[...])
        scores[pl.ds(start, tile), :] = s.reshape(tile, QUERIES)
        products[pl.ds(start, tile), :] = g
        g = g.reshape(tile // 8, 8, QUERIES)
        new = jnp.maximum(top, jnp.max(s, axis=0))
        shrink = jnp.exp2(top - new)
        p = jnp.exp2(s - new[None])
        total = total * shrink + jnp.sum(p, axis=0)
        delta = delta * shrink + jnp.sum(p * g, axis=0)
        return new, total, delta

    return lax.fori_loop(0, keys.shape[0] // tile, turn, running)


def first_kernel(where_ref, *refs):
    query_refs, key_refs = refs[0:8], refs[8:12]
    queries, grads, query_pos, keys, scores, products, out, values, key_pos = refs[12:]
    take_queries(where_ref, query_refs, queries, grads, query_pos)
    take_keys(where_ref, key_refs, keys, values, key_pos)
    start = (
        jnp.full((8, QUERIES), LOW, F32),
        jnp.zeros((8, QUERIES), F32),
        jnp.zeros((8, QUERIES), F32),
    )
    found = sweep(queries, grads, query_pos, keys, values, key_pos, scores, products, start)
    for n in range(3):
        out[n] = found[n]


def later_kernel(last, where_ref, *refs):
    queries, grads, query_pos, before = refs[0:4]
    if last:
        key_refs, refs = ((refs[4], refs[5]), (refs[6], refs[7])), refs[8:]
    else:
        key_refs, refs = refs[4:6], refs[6:]
    keys, scores, products, out, values, key_pos = refs
    take_keys(where_ref, key_refs, keys, values, key_pos)
    running = (before[0], before[1], before[2])
    top, total, delta = sweep(queries, grads, query_pos, keys, values, key_pos, scores, products, running)
    if not last:
        out[0], out[1], out[2] = top, total, delta
        return
    best = jnp.max(top, axis=0, keepdims=True)
    shrink = jnp.exp2(top - best)
    out[0:1, :] = best
    out[1:2, :] = jnp.sum(total * shrink, axis=0, keepdims=True)
    out[2:3, :] = jnp.sum(delta * shrink, axis=0, keepdims=True)
    out[3:8, :] = jnp.zeros((5, QUERIES), F32)


def grads_kernel(where_ref, *refs):
    queries, grads = refs[0:2]
    key_refs = refs[2:11]
    stat_refs = refs[11:15]
    own_query, query_outs = refs[15], refs[16:19]
    own_keys, key_outs = refs[19], refs[20:23]
    query_sum, query_rows = refs[23:]
    mine = where_ref[0]
    stats = [r[...] for r in stat_refs]
    tops = [s[0:1] for s in stats]
    best = functools.reduce(jnp.maximum, tops)
    shrinks = [jnp.exp2(t - best) for t in tops]
    total = sum(s[1:2] * w for s, w in zip(stats, shrinks))
    delta = sum(s[2:3] * w for s, w in zip(stats, shrinks)) / total
    log_total = jnp.broadcast_to(best + jnp.log2(total), (8, QUERIES))
    delta = jnp.broadcast_to(delta, (8, QUERIES))
    query_sum[...] = jnp.zeros_like(query_sum)
    for part, targets in enumerate(((own_keys, key_outs[0]), (key_outs[1],), (key_outs[2],))):
        keys, scores, products = key_refs[3 * part : 3 * part + 3]
        tile = tile_of(keys)
        for n in range(keys.shape[0] // tile):
            start = n * tile
            s = scores[start : start + tile, :].reshape(tile // 8, 8, QUERIES)
            g = products[start : start + tile, :].reshape(tile // 8, 8, QUERIES)
            p = jnp.exp2(s - log_total[None])
            d = (p * (g - delta[None])).reshape(tile, QUERIES).astype(BF16)
            p = p.reshape(tile, QUERIES).astype(BF16)
            grad_value = jnp.dot(p, grads[...], preferred_element_type=F32)
            grad_key = jnp.dot(d, queries[...], preferred_element_type=F32) * SCALE
            keys_t = jnp.transpose(keys[start : start + tile, :])
            query_sum[...] += jnp.dot(keys_t, d, preferred_element_type=F32)
            at = 0
            while at < tile:
                row = start + at
                chunk, inside = row // BOTH, row % BOTH
                size = min(tile - at, BOTH - inside)
                target = targets[chunk]
                target[inside : inside + size, :] = grad_key[at : at + size].astype(target.dtype)
                target[BOTH + inside : BOTH + inside + size, :] = grad_value[at : at + size].astype(target.dtype)
                at += size
    query_rows[...] = jnp.transpose(query_sum[...]) * SCALE
    for t in range(QUAD):
        rows = query_rows[pl.ds(pl.multiple_of((mine ^ t) * BOTH, BOTH), BOTH), :]
        if t == 0:
            own_query[...] = rows
        else:
            query_outs[t - 1][...] = rows.astype(BF16)


def in_vmem(n):
    return [pl.BlockSpec(memory_space=pltpu.VMEM)] * n


def shaped(*shape, dtype=BF16):
    return jax.ShapeDtypeStruct(shape, dtype)


def call(kernel, outs, scratch, flops, mib, where, *args):
    return pl.pallas_call(
        kernel,
        out_shape=tuple(outs),
        in_specs=[pl.BlockSpec(memory_space=pltpu.SMEM)] + in_vmem(len(args)),
        out_specs=tuple(in_vmem(len(outs))),
        scratch_shapes=scratch,
        compiler_params=pltpu.CompilerParams(vmem_limit_bytes=mib * 1024 * 1024),
        cost_estimate=pl.CostEstimate(flops=flops, bytes_accessed=4 * 10**6, transcendentals=0),
    )(where, *args)


def heads_of_own_rows(value, core):
    kept = lax.dynamic_index_in_dim(value, core, 0, False)
    sent = lax.dynamic_index_in_dim(value, 1 - core, 0, False)
    came = move(sent, xor_core=1)
    first = jnp.where(core == 0, kept, came)
    last = jnp.where(core == 0, came, kept)
    return jnp.concatenate([first, last], axis=-1)


def body(query_rows, key_rows, value_rows, grad_output, positions):
    place = lax.axis_index("seq")
    core = place % 2
    where = jnp.stack([(place // 16) * 2 + (place // 2) % 2, core]).astype(jnp.int32)
    key_pack = pack(key_rows, value_rows, positions)
    query_pack = pack(query_rows, grad_output, positions)
    key_near = {t: move(key_pack, xor_j=t) for t in (1, 3)}
    query_z = move(query_pack, xor_half=1)
    query_x = move(query_pack, xor_x=1)
    query_packs = [query_pack, query_z, query_x, move(query_z, xor_x=1)]
    head = move(key_near[3][: TAGS + ROWS], xor_j=1)
    tail = move(key_near[1][TAGS + ROWS :], xor_j=3)
    far_keys = (head, tail, move(head, xor_core=1), move(tail, xor_core=1))
    all_keys = [v for k in (key_pack, key_near[1], key_near[3]) for v in (k, move(k, xor_core=1))]
    all_queries = [v for q in query_packs for v in (q, move(q, xor_core=1))]

    rows = [shaped(QUERIES, 128), shaped(QUERIES, 128), shaped(8, QUERIES, dtype=F32)]

    def part_of(rows):
        outs = [shaped(rows, 128), *[shaped(rows, QUERIES, dtype=F32)] * 2]
        return outs, [pltpu.VMEM((rows, 128), BF16), pltpu.VMEM((rows, 128), F32)]

    running = shaped(3, 8, QUERIES, dtype=F32)
    outs, spare = part_of(2 * BOTH)
    *taken, keys_a, scores_a, products_a, found = call(
        first_kernel, rows + outs + [running], spare, 2 * 10**9, FIRST_MIB, where,
        *all_queries, *all_keys[:4],
    )
    outs, spare = part_of(BOTH)
    keys_c, scores_c, products_c, found = call(
        functools.partial(later_kernel, False), outs + [running], spare, 10**9, FIRST_MIB, where,
        *taken, found, *all_keys[4:6],
    )
    keys_b, scores_b, products_b, stats = call(
        functools.partial(later_kernel, True), outs + [shaped(8, QUERIES, dtype=F32)], spare, 10**9, FIRST_MIB,
        where, *taken, found, *far_keys,
    )
    all_stats = [stats] + [near_move(stats, t) for t in range(1, QUAD)]
    outs = call(
        grads_kernel,
        [shaped(BOTH, 128, dtype=F32)] + [shaped(BOTH, 128)] * 3
        + [shaped(2 * BOTH, 128, dtype=F32)] + [shaped(2 * BOTH, 128)] * 3,
        [pltpu.VMEM((128, QUERIES), F32), pltpu.VMEM((QUERIES, 128), F32)], 6 * 10**9, GRADS_MIB, where,
        *taken[:2], keys_a, scores_a, products_a, keys_c, scores_c, products_c, keys_b, scores_b, products_b, *all_stats,
    )
    own_query, query_outs, own_keys, key_outs = outs[0], outs[1:4], outs[4], outs[5:8]
    query_terms = [near_move(query_outs[t - 1], t) for t in range(1, QUAD)]
    key_terms = [move(out, xor_j=t) for out, t in zip(key_outs, (1, MID, LAST))]
    grad_query = (own_query + sum(t.astype(F32) for t in query_terms)).astype(BF16)
    grad_query = heads_of_own_rows(grad_query.reshape(2, ROWS, 128), core)
    regrouped = lax.all_to_all(grad_query.reshape(8, 24, 256), "head", 0, 0)
    regrouped = jnp.swapaxes(regrouped, 0, 1).reshape(24, 2048)
    both = (own_keys + sum(t.astype(F32) for t in key_terms)).astype(BF16)
    both = both.reshape(2, 2, ROWS, 128)
    grad_keys, grad_values = heads_of_own_rows(jnp.swapaxes(both, 0, 1), core)
    return regrouped, grad_keys, grad_values


def solution(mesh):
    placed = (P("seq", "head"), P("seq", "head"), P("seq", "head"), P("seq", "head"), P("seq"))
    return jax.shard_map(
        body,
        mesh=mesh,
        in_specs=placed,
        out_specs=(P(("seq", "head"), None), P("seq", "head"), P("seq", "head")),
        check_vma=False,
    )
```

```python
import functools

import jax
import jax.numpy as jnp
from jax import lax
from jax.experimental import pallas as pl
from jax.experimental.pallas import tpu as pltpu
from jax.sharding import PartitionSpec as P

HEAD_DIM = 128
ROWS = 192
TAGS = 16
BOTH = 2 * ROWS
QUAD = 4
QUERIES = QUAD * BOTH
MID, LAST = 3, 2
FIRST_MIB = 16
GRADS_MIB = 16
LOG2E = 1.4426950408889634
SCALE = HEAD_DIM**-0.5
LOW = -1e30
F32 = jnp.float32
BF16 = jnp.bfloat16


def z_of(j, half):
    return 2 * j + half


def perm(xor_x=0, xor_j=0, xor_half=0, xor_core=0):
    pairs = []
    for x in range(2):
        for j in range(4):
            for h in range(2):
                for c in range(2):
                    src = x * 16 + z_of(j, h) * 2 + c
                    dst = (x ^ xor_x) * 16 + z_of(j ^ xor_j, h ^ xor_half) * 2 + (c ^ xor_core)
                    pairs.append((src, dst))
    return pairs


def move(value, **how):
    return lax.ppermute(value, "seq", perm(**how))


def near_move(value, t):
    return move(value, xor_x=t // 2, xor_half=t % 2)


def pack(first, second, positions):
    high = (positions // 128).astype(BF16)
    low = (positions % 128).astype(BF16)
    tags = jnp.stack([high, low])
    tags = jnp.pad(tags, ((0, 0), (0, 2 * HEAD_DIM - ROWS)))
    tags = jnp.broadcast_to(tags[:, None, :], (2, 8, 2 * HEAD_DIM)).reshape(16, 2 * HEAD_DIM)
    return jnp.concatenate([tags, first, second], axis=0)


def places(packed_ref):
    tags = packed_ref[0:TAGS, :].astype(F32)
    return tags[0:8] * 128.0 + tags[8:16]


def split(packed_ref, cols, first, second, start):
    if isinstance(packed_ref, tuple):
        head, tail, base = *packed_ref, 0
    else:
        head, tail, base = packed_ref, packed_ref, TAGS + ROWS
    first[pl.ds(start, ROWS), :] = head[TAGS : TAGS + ROWS, cols]
    second[pl.ds(start, ROWS), :] = tail[base : base + ROWS, cols]


def head_cols(core):
    return pl.ds(pl.multiple_of(core * HEAD_DIM, HEAD_DIM), HEAD_DIM)


def take_queries(where_ref, refs, queries, grads, query_pos):
    mine, core = where_ref[0], where_ref[1]
    lane = lax.broadcasted_iota(jnp.int32, (8, 128), 1)
    for t in range(QUAD):
        chip = (mine ^ t) * BOTH
        for far in range(2):
            start = pl.multiple_of(chip + (core ^ far) * ROWS, 64)
            split(refs[2 * t + far], head_cols(core), queries, grads, start)
        own, other = places(refs[2 * t]), places(refs[2 * t + 1])
        left = jnp.where(core == 0, own, other)
        right = jnp.where(core == 0, other, own)
        turned_a = pltpu.roll(right[:, 0:128], 64, 1)
        turned_b = pltpu.roll(right[:, 128:256], 64, 1)
        row = jnp.concatenate(
            [left[:, 0:128], jnp.where(lane < 64, left[:, 128:256], turned_a), jnp.where(lane < 64, turned_a, turned_b)],
            axis=1,
        )
        query_pos[:, pl.ds(pl.multiple_of(chip, 128), BOTH)] = row


def take_keys(where_ref, refs, keys, values, key_pos):
    core = where_ref[1]
    for n in range(len(refs)):
        start = pl.multiple_of((n // 2) * BOTH + (core ^ (n % 2)) * ROWS, 64)
        split(refs[n], head_cols(core), keys, values, start)
        tagged = refs[n][0] if isinstance(refs[n], tuple) else refs[n]
        tall = jnp.concatenate([places(tagged)] * 16, axis=0)
        key_pos[pl.ds(start, 128), :] = jnp.transpose(tall[:, 0:128])
        key_pos[pl.ds(start + 128, 64), :] = jnp.transpose(tall[:, 128:256])[0:64]


def tile_of(keys):
    return 256 if keys.shape[0] % 256 == 0 else 192


def dot_t(a, b):
    return lax.dot_general(a, b, (((1,), (1,)), ((), ())), preferred_element_type=F32)


def masked_scores(queries, keys, query_pos, key_pos, start, tile):
    s = dot_t(keys[pl.ds(start, tile), :], queries[...])
    s = s.reshape(tile // 8, 8, QUERIES) * (SCALE * LOG2E)
    place = key_pos[pl.ds(start, tile), :].reshape(tile // 8, 8, 128)
    place = jnp.concatenate([place] * (QUERIES // 128), axis=2)
    return jnp.where(place <= query_pos[...][None], s, LOW)


def sweep(queries, grads, query_pos, keys, values, key_pos, scores, products, running):
    tile = tile_of(keys)

    def turn(i, running):
        top, total, delta = running
        start = i * tile
        s = masked_scores(queries, keys, query_pos, key_pos, start, tile)
        g = dot_t(values[pl.ds(start, tile), :], grads[...])
        scores[pl.ds(start, tile), :] = s.reshape(tile, QUERIES)
        products[pl.ds(start, tile), :] = g
        g = g.reshape(tile // 8, 8, QUERIES)
        new = jnp.maximum(top, jnp.max(s, axis=0))
        shrink = jnp.exp2(top - new)
        p = jnp.exp2(s - new[None])
        total = total * shrink + jnp.sum(p, axis=0)
        delta = delta * shrink + jnp.sum(p * g, axis=0)
        return new, total, delta

    for i in range(keys.shape[0] // tile):
        running = turn(i, running)
    return running


def first_kernel(where_ref, *refs):
    query_refs, key_refs = refs[0:8], refs[8:12]
    queries, grads, query_pos, keys, scores, products, out, values, key_pos = refs[12:]
    take_queries(where_ref, query_refs, queries, grads, query_pos)
    take_keys(where_ref, key_refs, keys, values, key_pos)
    start = (
        jnp.full((8, QUERIES), LOW, F32),
        jnp.zeros((8, QUERIES), F32),
        jnp.zeros((8, QUERIES), F32),
    )
    found = sweep(queries, grads, query_pos, keys, values, key_pos, scores, products, start)
    for n in range(3):
        out[n] = found[n]


def later_kernel(last, where_ref, *refs):
    queries, grads, query_pos, before = refs[0:4]
    if last:
        key_refs, refs = ((refs[4], refs[5]), (refs[6], refs[7])), refs[8:]
    else:
        key_refs, refs = refs[4:6], refs[6:]
    keys, scores, products, out, values, key_pos = refs
    take_keys(where_ref, key_refs, keys, values, key_pos)
    running = (before[0], before[1], before[2])
    top, total, delta = sweep(queries, grads, query_pos, keys, values, key_pos, scores, products, running)
    if not last:
        out[0], out[1], out[2] = top, total, delta
        return
    best = jnp.max(top, axis=0, keepdims=True)
    shrink = jnp.exp2(top - best)
    out[0:1, :] = best
    out[1:2, :] = jnp.sum(total * shrink, axis=0, keepdims=True)
    out[2:3, :] = jnp.sum(delta * shrink, axis=0, keepdims=True)
    out[3:8, :] = jnp.zeros((5, QUERIES), F32)


def grads_kernel(where_ref, *refs):
    queries, grads = refs[0:2]
    key_refs = refs[2:11]
    stat_refs = refs[11:15]
    own_query, query_outs = refs[15], refs[16:19]
    own_keys, key_outs = refs[19], refs[20:23]
    query_sum, query_rows = refs[23:]
    mine = where_ref[0]
    stats = [r[...] for r in stat_refs]
    tops = [s[0:1] for s in stats]
    best = functools.reduce(jnp.maximum, tops)
    shrinks = [jnp.exp2(t - best) for t in tops]
    total = sum(s[1:2] * w for s, w in zip(stats, shrinks))
    delta = sum(s[2:3] * w for s, w in zip(stats, shrinks)) / total
    log_total = jnp.broadcast_to(best + jnp.log2(total), (8, QUERIES))
    delta = jnp.broadcast_to(delta, (8, QUERIES))
    query_sum[...] = jnp.zeros_like(query_sum)
    for part, targets in enumerate(((own_keys, key_outs[0]), (key_outs[1],), (key_outs[2],))):
        keys, scores, products = key_refs[3 * part : 3 * part + 3]
        tile = tile_of(keys)
        for n in range(keys.shape[0] // tile):
            start = n * tile
            s = scores[start : start + tile, :].reshape(tile // 8, 8, QUERIES)
            g = products[start : start + tile, :].reshape(tile // 8, 8, QUERIES)
            p = jnp.exp2(s - log_total[None])
            d = (p * (g - delta[None])).reshape(tile, QUERIES).astype(BF16)
            p = p.reshape(tile, QUERIES).astype(BF16)
            grad_value = jnp.dot(p, grads[...], preferred_element_type=F32)
            grad_key = jnp.dot(d, queries[...], preferred_element_type=F32) * SCALE
            keys_t = jnp.transpose(keys[start : start + tile, :])
            query_sum[...] += jnp.dot(keys_t, d, preferred_element_type=F32)
            at = 0
            while at < tile:
                row = start + at
                chunk, inside = row // BOTH, row % BOTH
                size = min(tile - at, BOTH - inside)
                target = targets[chunk]
                target[inside : inside + size, :] = grad_key[at : at + size].astype(target.dtype)
                target[BOTH + inside : BOTH + inside + size, :] = grad_value[at : at + size].astype(target.dtype)
                at += size
    query_rows[...] = jnp.transpose(query_sum[...]) * SCALE
    for t in range(QUAD):
        rows = query_rows[pl.ds(pl.multiple_of((mine ^ t) * BOTH, BOTH), BOTH), :]
        if t == 0:
            own_query[...] = rows
        else:
            query_outs[t - 1][...] = rows.astype(BF16)


def in_vmem(n):
    return [pl.BlockSpec(memory_space=pltpu.VMEM)] * n


def shaped(*shape, dtype=BF16):
    return jax.ShapeDtypeStruct(shape, dtype)


def call(kernel, outs, scratch, flops, mib, where, *args):
    return pl.pallas_call(
        kernel,
        out_shape=tuple(outs),
        in_specs=[pl.BlockSpec(memory_space=pltpu.SMEM)] + in_vmem(len(args)),
        out_specs=tuple(in_vmem(len(outs))),
        scratch_shapes=scratch,
        compiler_params=pltpu.CompilerParams(vmem_limit_bytes=mib * 1024 * 1024),
        cost_estimate=pl.CostEstimate(flops=flops, bytes_accessed=4 * 10**6, transcendentals=0),
    )(where, *args)


def heads_of_own_rows(value, core):
    kept = lax.dynamic_index_in_dim(value, core, 0, False)
    sent = lax.dynamic_index_in_dim(value, 1 - core, 0, False)
    came = move(sent, xor_core=1)
    first = jnp.where(core == 0, kept, came)
    last = jnp.where(core == 0, came, kept)
    return jnp.concatenate([first, last], axis=-1)


def body(query_rows, key_rows, value_rows, grad_output, positions):
    place = lax.axis_index("seq")
    core = place % 2
    where = jnp.stack([(place // 16) * 2 + (place // 2) % 2, core]).astype(jnp.int32)
    key_pack = pack(key_rows, value_rows, positions)
    query_pack = pack(query_rows, grad_output, positions)
    key_near = {t: move(key_pack, xor_j=t) for t in (1, 3)}
    query_z = move(query_pack, xor_half=1)
    query_x = move(query_pack, xor_x=1)
    query_packs = [query_pack, query_z, query_x, move(query_z, xor_x=1)]
    head = move(key_near[3][: TAGS + ROWS], xor_j=1)
    tail = move(key_near[1][TAGS + ROWS :], xor_j=3)
    far_keys = (head, tail, move(head, xor_core=1), move(tail, xor_core=1))
    all_keys = [v for k in (key_pack, key_near[1], key_near[3]) for v in (k, move(k, xor_core=1))]
    all_queries = [v for q in query_packs for v in (q, move(q, xor_core=1))]

    rows = [shaped(QUERIES, 128), shaped(QUERIES, 128), shaped(8, QUERIES, dtype=F32)]

    def part_of(rows):
        outs = [shaped(rows, 128), *[shaped(rows, QUERIES, dtype=F32)] * 2]
        return outs, [pltpu.VMEM((rows, 128), BF16), pltpu.VMEM((rows, 128), F32)]

    running = shaped(3, 8, QUERIES, dtype=F32)
    outs, spare = part_of(2 * BOTH)
    *taken, keys_a, scores_a, products_a, found = call(
        first_kernel, rows + outs + [running], spare, 2 * 10**9, FIRST_MIB, where,
        *all_queries, *all_keys[:4],
    )
    outs, spare = part_of(BOTH)
    keys_c, scores_c, products_c, found = call(
        functools.partial(later_kernel, False), outs + [running], spare, 10**9, FIRST_MIB, where,
        *taken, found, *all_keys[4:6],
    )
    keys_b, scores_b, products_b, stats = call(
        functools.partial(later_kernel, True), outs + [shaped(8, QUERIES, dtype=F32)], spare, 10**9, FIRST_MIB,
        where, *taken, found, *far_keys,
    )
    all_stats = [stats] + [near_move(stats, t) for t in range(1, QUAD)]
    outs = call(
        grads_kernel,
        [shaped(BOTH, 128, dtype=F32)] + [shaped(BOTH, 128)] * 3
        + [shaped(2 * BOTH, 128, dtype=F32)] + [shaped(2 * BOTH, 128)] * 3,
        [pltpu.VMEM((128, QUERIES), F32), pltpu.VMEM((QUERIES, 128), F32)], 6 * 10**9, GRADS_MIB, where,
        *taken[:2], keys_a, scores_a, products_a, keys_c, scores_c, products_c, keys_b, scores_b, products_b, *all_stats,
    )
    own_query, query_outs, own_keys, key_outs = outs[0], outs[1:4], outs[4], outs[5:8]
    query_terms = [near_move(query_outs[t - 1], t) for t in range(1, QUAD)]
    key_terms = [move(out, xor_j=t) for out, t in zip(key_outs, (1, MID, LAST))]
    grad_query = (own_query + sum(t.astype(F32) for t in query_terms)).astype(BF16)
    grad_query = heads_of_own_rows(grad_query.reshape(2, ROWS, 128), core)
    regrouped = lax.all_to_all(grad_query.reshape(8, 24, 256), "head", 0, 0)
    regrouped = jnp.swapaxes(regrouped, 0, 1).reshape(24, 2048)
    both = (own_keys + sum(t.astype(F32) for t in key_terms)).astype(BF16)
    both = both.reshape(2, 2, ROWS, 128)
    grad_keys, grad_values = heads_of_own_rows(jnp.swapaxes(both, 0, 1), core)
    return regrouped, grad_keys, grad_values


def solution(mesh):
    placed = (P("seq", "head"), P("seq", "head"), P("seq", "head"), P("seq", "head"), P("seq"))
    return jax.shard_map(
        body,
        mesh=mesh,
        in_specs=placed,
        out_specs=(P(("seq", "head"), None), P("seq", "head"), P("seq", "head")),
        check_vma=False,
    )
```

```python
import functools

import jax
import jax.numpy as jnp
from jax import lax
from jax.experimental import pallas as pl
from jax.experimental.pallas import tpu as pltpu
from jax.sharding import PartitionSpec as P

HEAD_DIM = 128
ROWS = 192
TAGS = 16
BOTH = 2 * ROWS
QUAD = 4
QUERIES = QUAD * BOTH
HALF = QUERIES // 2
MID, LAST = 3, 2
FIRST_MIB = 16
GRADS_MIB = 16
LOG2E = 1.4426950408889634
SCALE = HEAD_DIM**-0.5
LOW = -1e30
F32 = jnp.float32
BF16 = jnp.bfloat16


def z_of(j, half):
    return 2 * j + half


def perm(xor_x=0, xor_j=0, xor_half=0, xor_core=0):
    pairs = []
    for x in range(2):
        for j in range(4):
            for h in range(2):
                for c in range(2):
                    src = x * 16 + z_of(j, h) * 2 + c
                    dst = (x ^ xor_x) * 16 + z_of(j ^ xor_j, h ^ xor_half) * 2 + (c ^ xor_core)
                    pairs.append((src, dst))
    return pairs


def move(value, **how):
    return lax.ppermute(value, "seq", perm(**how))


def near_move(value, t):
    return move(value, xor_x=t // 2, xor_half=t % 2)


def pack(first, second, positions):
    high = (positions // 128).astype(BF16)
    low = (positions % 128).astype(BF16)
    tags = jnp.stack([high, low])
    tags = jnp.pad(tags, ((0, 0), (0, 2 * HEAD_DIM - ROWS)))
    tags = jnp.broadcast_to(tags[:, None, :], (2, 8, 2 * HEAD_DIM)).reshape(16, 2 * HEAD_DIM)
    return jnp.concatenate([tags, first, second], axis=0)


def places(packed_ref):
    tags = packed_ref[0:TAGS, :].astype(F32)
    return tags[0:8] * 128.0 + tags[8:16]


def split(packed_ref, cols, first, second, start):
    if isinstance(packed_ref, tuple):
        head, tail, base = *packed_ref, 0
    else:
        head, tail, base = packed_ref, packed_ref, TAGS + ROWS
    first[pl.ds(start, ROWS), :] = head[TAGS : TAGS + ROWS, cols]
    second[pl.ds(start, ROWS), :] = tail[base : base + ROWS, cols]


def head_cols(core):
    return pl.ds(pl.multiple_of(core * HEAD_DIM, HEAD_DIM), HEAD_DIM)


def take_queries(where_ref, refs, queries, grads, query_pos):
    mine, core = where_ref[0], where_ref[1]
    lane = lax.broadcasted_iota(jnp.int32, (8, 128), 1)
    for t in range(QUAD):
        chip = (mine ^ t) * BOTH
        for far in range(2):
            start = pl.multiple_of(chip + (core ^ far) * ROWS, 64)
            split(refs[2 * t + far], head_cols(core), queries, grads, start)
        own, other = places(refs[2 * t]), places(refs[2 * t + 1])
        left = jnp.where(core == 0, own, other)
        right = jnp.where(core == 0, other, own)
        turned_a = pltpu.roll(right[:, 0:128], 64, 1)
        turned_b = pltpu.roll(right[:, 128:256], 64, 1)
        row = jnp.concatenate(
            [left[:, 0:128], jnp.where(lane < 64, left[:, 128:256], turned_a), jnp.where(lane < 64, turned_a, turned_b)],
            axis=1,
        )
        query_pos[:, pl.ds(pl.multiple_of(chip, 128), BOTH)] = row


def take_keys(where_ref, refs, keys, values, key_pos):
    core = where_ref[1]
    for n in range(len(refs)):
        start = pl.multiple_of((n // 2) * BOTH + (core ^ (n % 2)) * ROWS, 64)
        split(refs[n], head_cols(core), keys, values, start)
        tagged = refs[n][0] if isinstance(refs[n], tuple) else refs[n]
        tall = jnp.concatenate([places(tagged)] * 16, axis=0)
        key_pos[pl.ds(start, 128), :] = jnp.transpose(tall[:, 0:128])
        key_pos[pl.ds(start + 128, 64), :] = jnp.transpose(tall[:, 128:256])[0:64]


def tile_of(keys):
    return 256 if keys.shape[0] % 256 == 0 else 192


def dot_t(a, b):
    return lax.dot_general(a, b, (((1,), (1,)), ((), ())), preferred_element_type=F32)


def masked_scores(queries, keys, query_pos, key_pos, start, tile):
    s = dot_t(keys[pl.ds(start, tile), :], queries[...])
    s = s.reshape(tile // 8, 8, QUERIES) * (SCALE * LOG2E)
    place = key_pos[pl.ds(start, tile), :].reshape(tile // 8, 8, 128)
    place = jnp.concatenate([place] * (QUERIES // 128), axis=2)
    return jnp.where(place <= query_pos[...][None], s, LOW)


def sweep(queries, grads, query_pos, keys, values, key_pos, scores, products, running):
    tile = tile_of(keys)

    def turn(i, running):
        top, total, delta = running
        start = i * tile
        s = masked_scores(queries, keys, query_pos, key_pos, start, tile)
        g = dot_t(values[pl.ds(start, tile), :], grads[...])
        scores[pl.ds(start, tile), :] = s.reshape(tile, QUERIES)
        products[pl.ds(start, tile), :] = g
        g = g.reshape(tile // 8, 8, QUERIES)
        new = jnp.maximum(top, jnp.max(s, axis=0))
        shrink = jnp.exp2(top - new)
        p = jnp.exp2(s - new[None])
        total = total * shrink + jnp.sum(p, axis=0)
        delta = delta * shrink + jnp.sum(p * g, axis=0)
        return new, total, delta

    for i in range(keys.shape[0] // tile):
        running = turn(i, running)
    return running


def first_kernel(where_ref, *refs):
    query_refs, key_refs = refs[0:8], refs[8:12]
    queries, grads, query_pos, keys, scores, products, out, values, key_pos = refs[12:]
    take_queries(where_ref, query_refs, queries, grads, query_pos)
    take_keys(where_ref, key_refs, keys, values, key_pos)
    start = (
        jnp.full((8, QUERIES), LOW, F32),
        jnp.zeros((8, QUERIES), F32),
        jnp.zeros((8, QUERIES), F32),
    )
    found = sweep(queries, grads, query_pos, keys, values, key_pos, scores, products, start)
    for n in range(3):
        out[n] = found[n]


def later_kernel(last, where_ref, *refs):
    queries, grads, query_pos, before = refs[0:4]
    if last:
        key_refs, refs = ((refs[4], refs[5]), (refs[6], refs[7])), refs[8:]
    else:
        key_refs, refs = refs[4:6], refs[6:]
    keys, scores, products, out, values, key_pos = refs
    take_keys(where_ref, key_refs, keys, values, key_pos)
    running = (before[0], before[1], before[2])
    top, total, delta = sweep(queries, grads, query_pos, keys, values, key_pos, scores, products, running)
    if not last:
        out[0], out[1], out[2] = top, total, delta
        return
    best = jnp.max(top, axis=0, keepdims=True)
    shrink = jnp.exp2(top - best)
    sums = [jnp.sum(v * shrink, axis=0, keepdims=True) for v in (total, delta)]
    for n, row in enumerate((best, *sums)):
        for part in range(2):
            out[2 * n + part : 2 * n + part + 1, :] = row[:, part * HALF : (part + 1) * HALF]
    out[6:8, :] = jnp.zeros((2, HALF), F32)


def grads_kernel(where_ref, *refs):
    queries, grads = refs[0:2]
    key_refs = refs[2:11]
    stat_refs = refs[11:15]
    own_query, query_outs = refs[15], refs[16:19]
    own_keys, key_outs = refs[19], refs[20:23]
    query_sum, query_rows = refs[23:]
    mine = where_ref[0]
    stats = [[jnp.concatenate([r[2 * n : 2 * n + 1, :], r[2 * n + 1 : 2 * n + 2, :]], axis=1) for n in range(3)] for r in stat_refs]
    tops = [s[0] for s in stats]
    best = functools.reduce(jnp.maximum, tops)
    shrinks = [jnp.exp2(t - best) for t in tops]
    total = sum(s[1] * w for s, w in zip(stats, shrinks))
    delta = sum(s[2] * w for s, w in zip(stats, shrinks)) / total
    log_total = jnp.broadcast_to(best + jnp.log2(total), (8, QUERIES))
    delta = jnp.broadcast_to(delta, (8, QUERIES))
    query_sum[...] = jnp.zeros_like(query_sum)
    for part, targets in enumerate(((own_keys, key_outs[0]), (key_outs[1],), (key_outs[2],))):
        keys, scores, products = key_refs[3 * part : 3 * part + 3]
        tile = tile_of(keys)
        for n in range(keys.shape[0] // tile):
            start = n * tile
            s = scores[start : start + tile, :].reshape(tile // 8, 8, QUERIES)
            g = products[start : start + tile, :].reshape(tile // 8, 8, QUERIES)
            p = jnp.exp2(s - log_total[None])
            d = (p * (g - delta[None])).reshape(tile, QUERIES).astype(BF16)
            p = p.reshape(tile, QUERIES).astype(BF16)
            grad_value = jnp.dot(p, grads[...], preferred_element_type=F32)
            grad_key = jnp.dot(d, queries[...], preferred_element_type=F32) * SCALE
            keys_t = jnp.transpose(keys[start : start + tile, :])
            query_sum[...] += jnp.dot(keys_t, d, preferred_element_type=F32)
            at = 0
            while at < tile:
                row = start + at
                chunk, inside = row // BOTH, row % BOTH
                size = min(tile - at, BOTH - inside)
                target = targets[chunk]
                target[inside : inside + size, :] = grad_key[at : at + size].astype(target.dtype)
                target[BOTH + inside : BOTH + inside + size, :] = grad_value[at : at + size].astype(target.dtype)
                at += size
    query_rows[...] = jnp.transpose(query_sum[...]) * SCALE
    for t in range(QUAD):
        rows = query_rows[pl.ds(pl.multiple_of((mine ^ t) * BOTH, BOTH), BOTH), :]
        if t == 0:
            own_query[...] = rows
        else:
            query_outs[t - 1][...] = rows.astype(BF16)


def in_vmem(n):
    return [pl.BlockSpec(memory_space=pltpu.VMEM)] * n


def shaped(*shape, dtype=BF16):
    return jax.ShapeDtypeStruct(shape, dtype)


def call(kernel, outs, scratch, flops, mib, where, *args):
    return pl.pallas_call(
        kernel,
        out_shape=tuple(outs),
        in_specs=[pl.BlockSpec(memory_space=pltpu.SMEM)] + in_vmem(len(args)),
        out_specs=tuple(in_vmem(len(outs))),
        scratch_shapes=scratch,
        compiler_params=pltpu.CompilerParams(vmem_limit_bytes=mib * 1024 * 1024),
        cost_estimate=pl.CostEstimate(flops=flops, bytes_accessed=4 * 10**6, transcendentals=0),
    )(where, *args)


def heads_of_own_rows(value, core):
    kept = lax.dynamic_index_in_dim(value, core, 0, False)
    sent = lax.dynamic_index_in_dim(value, 1 - core, 0, False)
    came = move(sent, xor_core=1)
    first = jnp.where(core == 0, kept, came)
    last = jnp.where(core == 0, came, kept)
    return jnp.concatenate([first, last], axis=-1)


def body(query_rows, key_rows, value_rows, grad_output, positions):
    place = lax.axis_index("seq")
    core = place % 2
    where = jnp.stack([(place // 16) * 2 + (place // 2) % 2, core]).astype(jnp.int32)
    key_pack = pack(key_rows, value_rows, positions)
    query_pack = pack(query_rows, grad_output, positions)
    key_near = {t: move(key_pack, xor_j=t) for t in (1, 3)}
    query_z = move(query_pack, xor_half=1)
    query_x = move(query_pack, xor_x=1)
    query_packs = [query_pack, query_z, query_x, move(query_z, xor_x=1)]
    head = move(key_near[3][: TAGS + ROWS], xor_j=1)
    tail = move(key_near[1][TAGS + ROWS :], xor_j=3)
    far_keys = (head, tail, move(head, xor_core=1), move(tail, xor_core=1))
    all_keys = [v for k in (key_pack, key_near[1], key_near[3]) for v in (k, move(k, xor_core=1))]
    all_queries = [v for q in query_packs for v in (q, move(q, xor_core=1))]

    rows = [shaped(QUERIES, 128), shaped(QUERIES, 128), shaped(8, QUERIES, dtype=F32)]

    def part_of(rows):
        outs = [shaped(rows, 128), *[shaped(rows, QUERIES, dtype=F32)] * 2]
        return outs, [pltpu.VMEM((rows, 128), BF16), pltpu.VMEM((rows, 128), F32)]

    running = shaped(3, 8, QUERIES, dtype=F32)
    outs, spare = part_of(2 * BOTH)
    *taken, keys_a, scores_a, products_a, found = call(
        first_kernel, rows + outs + [running], spare, 2 * 10**9, FIRST_MIB, where,
        *all_queries, *all_keys[:4],
    )
    outs, spare = part_of(BOTH)
    keys_c, scores_c, products_c, found = call(
        functools.partial(later_kernel, False), outs + [running], spare, 10**9, FIRST_MIB, where,
        *taken, found, *all_keys[4:6],
    )
    keys_b, scores_b, products_b, stats = call(
        functools.partial(later_kernel, True), outs + [shaped(8, HALF, dtype=F32)], spare, 10**9, FIRST_MIB,
        where, *taken, found, *far_keys,
    )
    all_stats = [stats] + [near_move(stats, t) for t in range(1, QUAD)]
    outs = call(
        grads_kernel,
        [shaped(BOTH, 128, dtype=F32)] + [shaped(BOTH, 128)] * 3
        + [shaped(2 * BOTH, 128, dtype=F32)] + [shaped(2 * BOTH, 128)] * 3,
        [pltpu.VMEM((128, QUERIES), F32), pltpu.VMEM((QUERIES, 128), F32)], 6 * 10**9, GRADS_MIB, where,
        *taken[:2], keys_a, scores_a, products_a, keys_c, scores_c, products_c, keys_b, scores_b, products_b, *all_stats,
    )
    own_query, query_outs, own_keys, key_outs = outs[0], outs[1:4], outs[4], outs[5:8]
    query_terms = [near_move(query_outs[t - 1], t) for t in range(1, QUAD)]
    key_terms = [move(out, xor_j=t) for out, t in zip(key_outs, (1, MID, LAST))]
    grad_query = (own_query + sum(t.astype(F32) for t in query_terms)).astype(BF16)
    grad_query = heads_of_own_rows(grad_query.reshape(2, ROWS, 128), core)
    regrouped = lax.all_to_all(grad_query.reshape(8, 24, 256), "head", 0, 0)
    regrouped = jnp.swapaxes(regrouped, 0, 1).reshape(24, 2048)
    both = (own_keys + sum(t.astype(F32) for t in key_terms)).astype(BF16)
    both = both.reshape(2, 2, ROWS, 128)
    grad_keys, grad_values = heads_of_own_rows(jnp.swapaxes(both, 0, 1), core)
    return regrouped, grad_keys, grad_values


def solution(mesh):
    placed = (P("seq", "head"), P("seq", "head"), P("seq", "head"), P("seq", "head"), P("seq"))
    return jax.shard_map(
        body,
        mesh=mesh,
        in_specs=placed,
        out_specs=(P(("seq", "head"), None), P("seq", "head"), P("seq", "head")),
        check_vma=False,
    )
```
